32 devices in a mesh: dp: 16 (over z, x, core), mp: 2 (over y).
Axes of the slice: x: 2, y: 2, z: 4, core: 2. Of those that a mesh axis runs over, the one named last changes fastest.
Arguments:
- tokens: bfloat16 [192, 4608], P('dp', 'mp'), may hold values from -6 to 6
- frozen_weight: bfloat16 [2, 4608, 36864], P(None, 'mp', 'dp'), may hold values from -36 to 36
- adapter_down: bfloat16 [2, 16, 4608], P(None, None, 'mp'), may hold values from -1.5 to 1.5
- adapter_up: bfloat16 [2, 16, 36864], P(None, None, 'dp'), may hold values from -3 to 3
- magnitude: float32 [2, 36864], P(None, 'dp'), may hold values from 0.5 to 2
- hidden_gradient: bfloat16 [192, 36864], P('mp', 'dp'), may hold values from -0.59765625 to 0.59765625
Outputs:
- hidden: bfloat16 [192, 36864], P('mp', 'dp')
- token_gradient: float32 [192, 4608], P('dp', 'mp')
- adapter_down_gradient: float32 [2, 16, 4608], P(None, None, 'mp')
- adapter_up_gradient: float32 [2, 16, 36864], P(None, None, 'dp')
- magnitude_gradient: float32 [2, 36864], P(None, 'dp')
The draws below stay inside these ranges and needn't reach their ends.
All inputs are finite; a program needn't handle non-finite values.
Results may differ from the reference program's by a relative error of at most 0.023.
Values may be sent and summed in bfloat16 or wider, within the bound.
A program may use at most 64 MiB of HBM per device.

```python
import math
import jax
import jax.numpy as jnp
from jax import lax

MODEL_WIDTH = 4608
HIDDEN_UNITS = 36864
ADAPTER_RANK = 16
TOKENS = 192
N_DP = 16
N_MP = 2


def draw_frozen_weight(key, part):
    row_key = jax.random.fold_in(key, 11)
    col_key = jax.random.fold_in(key, 12)
    entry_key = jax.random.fold_in(key, 13)
    positions = jnp.arange(MODEL_WIDTH, dtype=jnp.float32) / (MODEL_WIDTH - 1)
    row_ramp = jnp.sqrt(1.0 + 2.0 * positions).reshape(1, MODEL_WIDTH, 1)
    row_scale = row_ramp * jnp.exp(jax.random.uniform(row_key, (2, MODEL_WIDTH, 1), jnp.float32, 0.0, 1.7917595))
    col_scale = jnp.exp(jax.random.uniform(col_key, (2, 1, HIDDEN_UNITS), jnp.float32, -1.2039728, 1.0986123))
    entries = jnp.clip(jax.random.normal(entry_key, (2, MODEL_WIDTH, HIDDEN_UNITS), jnp.float32), -5.0, 5.0)
    return (entries * row_scale * col_scale / 4.4).astype(jnp.bfloat16)


def steps_of(key, dims, pieces, smallest, high):
    def one(dim, shards_of):
        draws = jax.random.uniform(jax.random.fold_in(jax.random.fold_in(key, 6), dim), (shards_of,), jnp.float32, smallest / len(pieces), high / len(pieces))
        return jnp.repeat(jnp.exp(draws), dims[dim] // shards_of).reshape((-1,) + (1,) * (len(dims) - dim - 1))

    gain = one(*pieces[0])
    for cut in pieces[1:]:
        gain = gain * one(*cut)
    return gain


def scatter_about(rng, shape, deviation, bound, cuts=(), kind=jnp.bfloat16):
    level = steps_of(rng, shape, cuts, -0.22, 0.18) if cuts else 1.0
    drawn = jax.random.normal(rng, shape, jnp.float32) * deviation * level
    return jnp.minimum(jnp.maximum(drawn, -bound), bound).astype(kind)


def setup_inputs(seed: int = 0) -> dict:
    key_of = jax.random.split(jax.random.key(seed), 7)
    tokens = scatter_about(key_of[0], (TOKENS, MODEL_WIDTH), 1.0, 6.0, ((0, 16), (1, 2)))
    frozen_weight = draw_frozen_weight(jax.random.fold_in(key_of[6], 71), 0)
    adapter_down = scatter_about(key_of[2], (2, ADAPTER_RANK, MODEL_WIDTH), ADAPTER_RANK ** -0.5, 1.5, ((2, 2),))
    adapter_up = scatter_about(key_of[3], (2, ADAPTER_RANK, HIDDEN_UNITS), 0.5, 3.0, ((2, 16),))
    magnitude = jnp.clip(jnp.exp(math.log(2.0) - 1.3862944 * jax.random.uniform(key_of[4], (2, HIDDEN_UNITS), jnp.float32) ** steps_of(key_of[4], (2, HIDDEN_UNITS), ((1, 16),), -0.2, 0.2)), 0.5, 2.0)
    hidden_gradient = scatter_about(key_of[5], (TOKENS, HIDDEN_UNITS), 0.1, 0.59765625, ((0, 2), (1, 16)))
    return {"tokens": tokens, "frozen_weight": frozen_weight, "adapter_down": adapter_down, "adapter_up": adapter_up, "magnitude": magnitude, "hidden_gradient": hidden_gradient}


LOWRANK_SCALE = 2.0
EPSILON = 1e-06
MATMUL_ACCURACY = lax.Precision.HIGHEST

def gelu_pair(source):
    cubic_term = source + 0.044715 * source * source * source
    tangent = jnp.tanh(0.7978845608028654 * cubic_term)
    result = 0.5 * source * (1.0 + tangent)
    derivative = 0.5 * (1.0 + tangent) + 0.5 * source * (1.0 - tangent * tangent) * 0.7978845608028654 * (1.0 + 0.134145 * source * source)
    return (result, derivative)

def group_product(tokens, weights):
    group_depth = MODEL_WIDTH // N_MP
    col_count = weights.shape[2]

    def add_group(running, group_index):
        offset = group_index * group_depth
        token_cols = lax.dynamic_slice_in_dim(tokens, offset, group_depth, 1).astype(jnp.float32)
        weight_rows = lax.dynamic_slice_in_dim(weights, offset, group_depth, 1).astype(jnp.float32)
        partial_sum = jnp.einsum('td,kdf->ktf', token_cols, weight_rows, precision=MATMUL_ACCURACY)
        rounded = lax.optimization_barrier(partial_sum.astype(jnp.bfloat16))
        return (running + rounded.astype(jnp.float32), None)
    initial = jnp.zeros((2, TOKENS, col_count), jnp.float32)
    return lax.scan(add_group, initial, jnp.arange(N_MP, dtype=jnp.int32))[0]

def combined_block(frozen_block, adapter_down, adapter_up_block):
    lowrank_delta = jnp.einsum('ipq,iph->iqh', adapter_down.astype(jnp.float32), adapter_up_block.astype(jnp.float32), precision=MATMUL_ACCURACY)
    return frozen_block.astype(jnp.float32) + LOWRANK_SCALE * lowrank_delta

def reference(tokens, frozen_weight, adapter_down, adapter_up, magnitude, hidden_gradient):
    column_blocks = N_DP
    block_columns = HIDDEN_UNITS // column_blocks
    weight_blocks = jnp.moveaxis(frozen_weight.reshape(2, MODEL_WIDTH, column_blocks, block_columns), 2, 0)
    adapter_up_blocks = jnp.moveaxis(adapter_up.reshape(2, ADAPTER_RANK, column_blocks, block_columns), 2, 0)
    down_broad = adapter_down.astype(jnp.float32)

    def norm_pass(block_pieces):
        combined_weight = combined_block(block_pieces[0], adapter_down, block_pieces[1])
        squares = lax.optimization_barrier(jnp.sum(combined_weight * combined_weight, axis=1))
        cross_part = jnp.einsum('krd,kdf->krf', down_broad, combined_weight, precision=MATMUL_ACCURACY)
        return (squares, cross_part)
    squares, cross_parts = lax.map(norm_pass, (weight_blocks, adapter_up_blocks))
    square_sum = jnp.moveaxis(squares, 0, 1).reshape(2, HIDDEN_UNITS)
    mixed_sum = jnp.moveaxis(cross_parts, 0, 2).reshape(2, ADAPTER_RANK, HIDDEN_UNITS)
    col_norm = jnp.sqrt(square_sum + EPSILON)
    col_ratio = magnitude / col_norm
    token_lowrank = group_product(tokens, jnp.swapaxes(adapter_down, 1, 2)).astype(jnp.bfloat16)
    frozen_matrix = group_product(tokens, frozen_weight)
    unscaled_output = frozen_matrix + LOWRANK_SCALE * jnp.einsum('hls,hse->hle', token_lowrank.astype(jnp.float32), adapter_up.astype(jnp.float32), precision=MATMUL_ACCURACY)
    gate_proj = unscaled_output[0] * col_ratio[0]
    up_proj = unscaled_output[1] * col_ratio[1]
    activated, derivative = gelu_pair(gate_proj)
    hidden = (activated * up_proj).astype(jnp.bfloat16)
    cotangent = hidden_gradient.astype(jnp.float32)
    grad_out = jnp.stack([cotangent * up_proj * derivative, cotangent * activated])
    moment = lax.optimization_barrier(jnp.sum(grad_out * unscaled_output, axis=1))
    magnitude_gradient = moment / col_norm
    frozen_term = -magnitude * moment / (col_norm * col_norm * col_norm)
    prescale_gradient = (grad_out * col_ratio[:, None, :]).astype(jnp.bfloat16)
    lowrank_gradient = jnp.stack([jnp.dot(prescale_gradient[pair_member], adapter_up[pair_member].T, preferred_element_type=jnp.float32) for pair_member in range(2)]).astype(jnp.bfloat16)
    adapter_up_gradient = LOWRANK_SCALE * (jnp.einsum('hmu,hmq->huq', token_lowrank.astype(jnp.float32), prescale_gradient.astype(jnp.float32), precision=MATMUL_ACCURACY) + mixed_sum * frozen_term[:, None, :])
    weighted_adapter_up = adapter_up.astype(jnp.float32) * frozen_term[:, None, :]
    weighted_blocks = jnp.moveaxis(weighted_adapter_up.reshape(2, ADAPTER_RANK, column_blocks, block_columns), 2, 0)

    def spread_pass(running, block_pieces):
        combined_weight = combined_block(block_pieces[0], adapter_down, block_pieces[1])
        return (running + jnp.einsum('krf,kdf->krd', block_pieces[2], combined_weight, precision=MATMUL_ACCURACY), None)
    broadcast_value = lax.scan(spread_pass, jnp.zeros((2, ADAPTER_RANK, MODEL_WIDTH), jnp.float32), (weight_blocks, adapter_up_blocks, weighted_blocks))[0]
    adapter_down_gradient = LOWRANK_SCALE * (jnp.einsum('ijp,jv->ipv', lowrank_gradient.astype(jnp.float32), tokens.astype(jnp.float32), precision=MATMUL_ACCURACY) + broadcast_value)
    token_gradient = jnp.zeros((TOKENS, MODEL_WIDTH), jnp.float32)
    for pair_member in range(2):
        token_gradient = token_gradient + jnp.dot(prescale_gradient[pair_member], frozen_weight[pair_member].T, preferred_element_type=jnp.float32) + LOWRANK_SCALE * jnp.dot(lowrank_gradient[pair_member], adapter_down[pair_member], preferred_element_type=jnp.float32)
    return (hidden, token_gradient, adapter_down_gradient, adapter_up_gradient, magnitude_gradient)
```

```python
import functools

import jax
import jax.numpy as jnp
from jax import lax
from jax.experimental import pallas as pl
from jax.experimental.pallas import tpu as pltpu
from jax.sharding import PartitionSpec as P

LOWRANK_SCALE = 2.0
EPSILON = 1e-06
MATMUL_ACCURACY = lax.Precision.HIGHEST


def gelu_pair(source):
    cubic_term = source + 0.044715 * source * source * source
    tangent = jnp.tanh(0.7978845608028654 * cubic_term)
    result = 0.5 * source * (1.0 + tangent)
    derivative = 0.5 * (1.0 + tangent) + 0.5 * source * (
        1.0 - tangent * tangent
    ) * 0.7978845608028654 * (1.0 + 0.134145 * source * source)
    return (result, derivative)


def on_device(tokens, frozen_weight, adapter_down, adapter_up, magnitude, hidden_gradient):
    every_row = lax.all_gather(tokens, "dp", axis=0, tiled=True)
    down_broad = adapter_down.astype(jnp.float32)
    up_broad = adapter_up.astype(jnp.float32)
    base_square = jnp.sum(jnp.square(frozen_weight.astype(jnp.float32)), axis=1)
    cross_base = jnp.einsum(
        "krd,kdf->krf", adapter_down, frozen_weight, preferred_element_type=jnp.float32
    )
    gram_part = jnp.einsum(
        "krd,ksd->krs", adapter_down, adapter_down, preferred_element_type=jnp.float32
    )
    square_base, cross_total, gram_sum = (
        lax.psum(base_square.astype(jnp.bfloat16), "mp").astype(jnp.float32),
        lax.psum(cross_base.astype(jnp.bfloat16), "mp").astype(jnp.float32),
        lax.psum(gram_part.astype(jnp.bfloat16), "mp").astype(jnp.float32),
    )
    gram_up = jnp.einsum("krs,ksf->krf", gram_sum, up_broad, precision=MATMUL_ACCURACY)
    mixed_sum = cross_total + LOWRANK_SCALE * gram_up
    square_sum = (
        square_base
        + 2.0 * LOWRANK_SCALE * jnp.sum(up_broad * cross_total, axis=1)
        + LOWRANK_SCALE * LOWRANK_SCALE * jnp.sum(up_broad * gram_up, axis=1)
    )
    base_part = jnp.einsum(
        "td,kdf->ktf", every_row, frozen_weight, preferred_element_type=jnp.float32
    )
    lowrank_piece = jnp.einsum(
        "su,vgu->vsg", every_row, adapter_down, preferred_element_type=jnp.float32
    )
    col_norm = jnp.sqrt(square_sum + EPSILON)
    col_ratio = magnitude / col_norm
    share_rows = every_row.shape[0] // lax.axis_size("mp")
    base_sum, low_sum = (
        lax.psum(base_part.astype(jnp.bfloat16), "mp").astype(jnp.float32),
        lax.psum(lowrank_piece.astype(jnp.bfloat16), "mp").astype(jnp.float32),
    )
    cot_rows = lax.all_gather(hidden_gradient, "mp", axis=0, tiled=True)
    token_lowrank = low_sum.astype(jnp.bfloat16)
    unscaled_output = base_sum + LOWRANK_SCALE * jnp.einsum(
        "hls,hse->hle", token_lowrank, adapter_up, preferred_element_type=jnp.float32
    )
    gate_proj = unscaled_output[0] * col_ratio[0]
    up_proj = unscaled_output[1] * col_ratio[1]
    activated, derivative = gelu_pair(gate_proj)
    hidden_rows = (activated * up_proj).astype(jnp.bfloat16)
    cotangent = cot_rows.astype(jnp.float32)
    grad_out = jnp.stack([cotangent * up_proj * derivative, cotangent * activated])
    moment_part = jnp.sum(grad_out * unscaled_output, axis=1)
    prescale_gradient = (grad_out * col_ratio[:, None, :]).astype(jnp.bfloat16)
    lowrank_gradient_piece = jnp.einsum(
        "hmu,hmq->huq", token_lowrank, prescale_gradient, preferred_element_type=jnp.float32
    )
    hidden = lax.dynamic_slice_in_dim(hidden_rows, lax.axis_index("mp") * share_rows, share_rows, 0)
    magnitude_gradient = moment_part / col_norm
    frozen_term = -magnitude * moment_part / (col_norm * col_norm * col_norm)
    adapter_up_gradient = LOWRANK_SCALE * (
        lowrank_gradient_piece + mixed_sum * frozen_term[:, None, :]
    )
    lowrank_gradient = jnp.einsum(
        "pge,pbe->pgb", prescale_gradient, adapter_up, preferred_element_type=jnp.float32
    ).astype(jnp.bfloat16)
    weighted_adapter_up = up_broad * frozen_term[:, None, :]
    broadcast_value = jnp.einsum(
        "krf,kdf->krd",
        weighted_adapter_up,
        frozen_weight.astype(jnp.float32),
        precision=MATMUL_ACCURACY,
    )
    inner_gram = jnp.einsum(
        "krf,ksf->krs", weighted_adapter_up, up_broad, precision=MATMUL_ACCURACY
    )
    broadcast_value = broadcast_value + LOWRANK_SCALE * jnp.einsum(
        "krs,ksd->krd", inner_gram, down_broad, precision=MATMUL_ACCURACY
    )
    down_piece = LOWRANK_SCALE * (
        jnp.einsum("ijp,jv->ipv", lowrank_gradient, every_row, preferred_element_type=jnp.float32)
        + broadcast_value
    )
    adapter_down_gradient = lax.psum(down_piece, "dp")
    main_term = jnp.einsum(
        "ktf,kdf->td", prescale_gradient, frozen_weight, preferred_element_type=jnp.float32
    )
    token_gradient = lax.psum_scatter(
        main_term
        + LOWRANK_SCALE
        * jnp.einsum(
            "ijf,ifh->jh", lowrank_gradient, adapter_down, preferred_element_type=jnp.float32
        ),
        "dp",
        scatter_dimension=0,
        tiled=True,
    )
    return (hidden, token_gradient, adapter_down_gradient, adapter_up_gradient, magnitude_gradient)


MESH = pl.DeviceIdType.MESH
TILE = 256
LANES = 128
BLOCK = 16


def mm(left, right, precision=None):
    return lax.dot_general(
        left, right, (((1,), (0,)), ((), ())), precision=precision, preferred_element_type=jnp.float32
    )


def nt(left, right):
    return lax.dot_general(left, right, (((1,), (1,)), ((), ())), preferred_element_type=jnp.float32)


def fused_kernel(
    n_dp, chunks,
    tok, w, ad, up, mag, cot, gather_map, scatter_map,
    hid, tgrad, agrad, ugrad, mgrad,
    wv, tokpad, toks, mx_s, mx_r, sq_s, sq_r, tl_s, tl_r, tl_sum,
    base_s, base_o, base_r, gp, gr, mo, mr, lhs, tacc, aacc, glow, igram,
    blk, rsb, asum, agb,
    wsem, ag_ss, ag_rs, y_ss, y_rs, rs_ss, rs_rs, ah_ss, ah_rs,
):
    f32, bf16 = jnp.float32, jnp.bfloat16
    me = lax.axis_index("dp")
    mate = 1 - lax.axis_index("mp")
    rows, depth, width = tok.shape[0], w.shape[1], w.shape[2]
    rank = ad.shape[1]
    half = cot.shape[0]
    cw = width // chunks
    t = tgrad.shape[0]
    share = agrad.shape[1]

    loads = {}
    for c in range(chunks):
        for k in range(2):
            cut = pl.ds(c * cw, cw)
            copy = pltpu.make_async_copy(w.at[k, :, cut], wv.at[k, :, cut], wsem.at[c, k])
            copy.start()
            loads[c, k] = copy

    barrier = pltpu.get_barrier_semaphore()
    for i in range(1, n_dp):
        pl.semaphore_signal(barrier, inc=1, device_id={"dp": lax.rem(me + i, n_dp)}, device_id_type=MESH)
    pl.semaphore_signal(barrier, inc=1, device_id={"mp": mate}, device_id_type=MESH)
    pl.semaphore_wait(barrier, n_dp)

    def to_dp(source, target, ss, rs, i):
        return pltpu.make_async_remote_copy(
            src_ref=source, dst_ref=target, send_sem=ss.at[i], recv_sem=rs.at[i],
            device_id={"dp": lax.rem(me + i, n_dp)}, device_id_type=MESH,
        )

    used = []

    def to_mate(source, target):
        i = len(used)
        copy = pltpu.make_async_remote_copy(
            src_ref=source, dst_ref=target, send_sem=y_ss.at[i], recv_sem=y_rs.at[i],
            device_id={"mp": mate}, device_id_type=MESH,
        )
        used.append(copy)
        copy.start()
        return copy

    gathers = []
    for i in range(1, n_dp):
        copy = to_dp(tok, tokpad.at[me], ag_ss, ag_rs, i)
        copy.start()
        gathers.append(copy)
    tokpad[me] = tok[...]

    stats = []
    for c in range(chunks):
        for k in range(2):
            loads[c, k].wait()
            cols = pl.ds(c * cw, cw)

            def stat_step(r, carry):
                cross, square = carry
                at = pl.ds(pl.multiple_of(r * TILE, TILE), TILE)
                piece = wv[k, at, cols]
                wide = piece.astype(f32)
                cross = cross + mm(ad[k, :, at], piece)
                square = square + jnp.sum((wide * wide).reshape(TILE // 8, 8, cw), axis=0)
                return cross, square

            cross, square = lax.fori_loop(
                0, depth // TILE, stat_step, (jnp.zeros((rank, cw), f32), jnp.zeros((8, cw), f32))
            )
            gram = nt(ad[k], ad[k])
            up32 = up[k, :, cols].astype(f32)
            gram_up = mm(gram, up32, MATMUL_ACCURACY)
            total = (
                jnp.sum(square, axis=0, keepdims=True)
                + 2.0 * LOWRANK_SCALE * jnp.sum(up32 * cross, axis=0, keepdims=True)
                + LOWRANK_SCALE * LOWRANK_SCALE * jnp.sum(up32 * gram_up, axis=0, keepdims=True)
            )
            mx_s[c, k * rank : (k + 1) * rank, :] = (cross + LOWRANK_SCALE * gram_up).astype(bf16)
            sq_s[c, k : k + 1, :] = total
        stats.append((to_mate(mx_s.at[c], mx_r.at[c]), to_mate(sq_s.at[c], sq_r.at[c])))

    for copy in gathers:
        copy.wait()

    def gather_step(r, carry):
        at = pl.ds(pl.multiple_of(r * TILE, TILE), TILE)
        piece = tokpad[:, :, at].reshape(n_dp * BLOCK, TILE)
        toks[:, at] = mm(gather_map[...], piece).astype(bf16)
        return carry

    lax.fori_loop(0, depth // TILE, gather_step, 0)

    for k in range(2):
        low = nt(toks[...], ad[k]).astype(bf16)
        tl_s[0, k] = low[:half]
        tl_s[1, k] = low[half:]
    low_copy = to_mate(tl_s, tl_r)

    base_copies = []
    for c in range(chunks):

        def base_step(j, carry):
            at = pl.ds(pl.multiple_of(j * TILE, TILE), TILE)
            for k in range(2):
                piece = wv[k, :, pl.ds(pl.multiple_of(c * cw + j * TILE, TILE), TILE)]
                part = mm(toks[...], piece).astype(bf16)
                base_s[c, k, :, at] = part[:half]
                base_o[c, k, :, at] = part[half:]
            return carry

        lax.fori_loop(0, cw // TILE, base_step, 0)
        base_copies.append(to_mate(base_s.at[c], base_r.at[c]))

    low_copy.wait()
    for k in range(2):
        tl_sum[0, k] = (tl_s[0, k].astype(f32) + tl_r[1, k].astype(f32)).astype(bf16)
        tl_sum[1, k] = (tl_s[1, k].astype(f32) + tl_r[0, k].astype(f32)).astype(bf16)

    grads = []
    for c in range(chunks):
        for copy in stats[c]:
            copy.wait()
        base_copies[c].wait()

        def point_step(j, carry):
            at = pl.ds(pl.multiple_of(j * LANES, LANES), LANES)
            wide_at = pl.ds(pl.multiple_of(c * cw + j * LANES, LANES), LANES)
            pres, ratios = [], []
            for k in range(2):
                norm = jnp.sqrt(sq_s[c, k : k + 1, at] + sq_r[c, k : k + 1, at] + EPSILON)
                ratios.append(mag[k : k + 1, wide_at] / norm)
                base = base_o[c, k, :, at].astype(f32) + base_r[c, k, :, at].astype(f32)
                pres.append(base + LOWRANK_SCALE * mm(tl_sum[1, k], up[k, :, wide_at]))
            gate, upper = pres[0] * ratios[0], pres[1] * ratios[1]
            activated, derivative = gelu_pair(gate)
            hid[:, wide_at] = (activated * upper).astype(bf16)
            cotangent = cot[:, wide_at].astype(f32)
            outs = (cotangent * upper * derivative, cotangent * activated)
            for k in range(2):
                mo[c, k : k + 1, at] = jnp.sum(outs[k] * pres[k], axis=0, keepdims=True)
                gp[c, k, :, at] = (outs[k] * ratios[k]).astype(bf16)
            return carry

        lax.fori_loop(0, cw // LANES, point_step, 0)
        grads.append((to_mate(gp.at[c], gr.at[c]), to_mate(mo.at[c], mr.at[c])))

    for c in range(chunks):
        for copy in grads[c]:
            copy.wait()
        cols = pl.ds(c * cw, cw)
        for k in range(2):
            moment = mo[c, k : k + 1, :] + mr[c, k : k + 1, :]
            norm = jnp.sqrt(sq_s[c, k : k + 1, :] + sq_r[c, k : k + 1, :] + EPSILON)
            mgrad[k : k + 1, cols] = moment / norm
            frozen_term = -mag[k : k + 1, cols] * moment / (norm * norm * norm)
            part = pl.ds(k * rank, rank)
            mixed = mx_s[c, part, :].astype(f32) + mx_r[c, part, :].astype(f32)
            up16 = up[k, :, cols]
            weighted = up16.astype(f32) * frozen_term
            high = weighted.astype(bf16)
            low = (weighted - high.astype(f32)).astype(bf16)
            theirs, mine = gr[c, k], gp[c, k]
            piece = mm(tl_sum[0, k].astype(f32).T.astype(bf16), theirs) + mm(
                tl_sum[1, k].astype(f32).T.astype(bf16), mine
            )
            ugrad[k, :, cols] = LOWRANK_SCALE * (piece + mixed * frozen_term)
            lhs[k, 0:half, :] = theirs
            lhs[k, half : 2 * half, :] = mine
            lhs[k, 2 * half : 2 * half + rank, :] = high
            lhs[k, 2 * half + rank : 2 * half + 2 * rank, :] = low
            small = nt(lhs[k], up16)
            gl, ig = small[: 2 * half], small[2 * half : 2 * half + rank] + small[2 * half + rank :]
            if c == 0:
                glow[k] = gl
                igram[k] = ig
            else:
                glow[k] += gl
                igram[k] += ig

        def grad_step(r, carry):
            at = pl.ds(pl.multiple_of(r * TILE, TILE), TILE)
            outs = [nt(lhs[k], wv[k, at, cols]) for k in range(2)]
            main = outs[0][: 2 * half] + outs[1][: 2 * half]
            if c == 0:
                tacc[:, at] = main
            else:
                tacc[:, at] += main
            for k in range(2):
                spread = outs[k][2 * half : 2 * half + rank] + outs[k][2 * half + rank :]
                if c == 0:
                    aacc[k, :, at] = spread
                else:
                    aacc[k, :, at] += spread
            return carry

        lax.fori_loop(0, depth // TILE, grad_step, 0)

    def final_step(r, carry):
        at = pl.ds(pl.multiple_of(r * TILE, TILE), TILE)
        main = tacc[:, at]
        parts = []
        for k in range(2):
            low = glow[k].astype(bf16)
            adt = ad[k, :, at]
            main = main + LOWRANK_SCALE * mm(low, adt)
            spread = aacc[k, :, at] + LOWRANK_SCALE * mm(igram[k], adt.astype(f32), MATMUL_ACCURACY)
            parts.append(LOWRANK_SCALE * (mm(glow[k].T.astype(bf16), toks[:, at]) + spread))
        whole = jnp.concatenate([main] + parts, axis=0).astype(bf16)
        packed = mm(scatter_map[...], whole).astype(bf16)
        blk[:, :, at] = packed.reshape(n_dp, BLOCK, TILE)
        return carry

    lax.fori_loop(0, depth // TILE, final_step, 0)

    scatters = []
    for i in range(1, n_dp):
        copy = to_dp(blk.at[lax.rem(me + i, n_dp)], rsb.at[i], rs_ss, rs_rs, i)
        copy.start()
        scatters.append(copy)
    rsb[0] = blk[me]
    for copy in scatters:
        copy.wait()

    def sum_step(r, carry):
        at = pl.ds(pl.multiple_of(r * TILE, TILE), TILE)
        total = rsb[0, :, at].astype(f32)
        for i in range(1, n_dp):
            total = total + rsb[i, :, at].astype(f32)
        tgrad[:, at] = total[:t]
        asum[:, at] = total[t : t + share]
        return carry

    lax.fori_loop(0, depth // TILE, sum_step, 0)

    spreads = []
    for i in range(1, n_dp):
        copy = to_dp(asum, agb.at[me], ah_ss, ah_rs, i)
        copy.start()
        spreads.append(copy)
    agb[me] = asum[...]
    for copy in spreads:
        copy.wait()
    agrad[...] = agb[...]


def fused_on_device(n_dp, chunks, tokens, frozen_weight, adapter_down, adapter_up, magnitude, hidden_gradient):
    f32, bf16 = jnp.float32, jnp.bfloat16
    t, depth = tokens.shape
    rank, width = adapter_up.shape[1:]
    half = hidden_gradient.shape[0]
    count = n_dp * t
    share = 2 * rank // n_dp
    cw = width // chunks
    first = (1 - lax.axis_index("mp")) * half
    order = (jnp.arange(count) + first) % count
    places = (order // t) * BLOCK + order % t
    slots = jnp.arange(n_dp * BLOCK)
    gather_map = (places[:, None] == slots[None, :]).astype(bf16)
    spots = jnp.arange(2 * rank)
    spots = (spots // share) * BLOCK + t + spots % share
    scatter_map = (slots[:, None] == jnp.concatenate([places, spots])[None, :]).astype(bf16)
    padded = jnp.pad(tokens, ((0, BLOCK - t), (0, 0)))
    vmem = pl.BlockSpec(memory_space=pltpu.VMEM)
    dma = pltpu.SemaphoreType.DMA
    V = pltpu.VMEM
    messages = 5 * chunks + 1 + chunks
    hidden, tgrad, agrad, ugrad, mgrad = pl.pallas_call(
        functools.partial(fused_kernel, n_dp, chunks),
        out_shape=(
            jax.ShapeDtypeStruct((half, width), bf16),
            jax.ShapeDtypeStruct((t, depth), f32),
            jax.ShapeDtypeStruct((n_dp, share, depth), f32),
            jax.ShapeDtypeStruct((2, rank, width), f32),
            jax.ShapeDtypeStruct((2, width), f32),
        ),
        in_specs=[vmem, pl.BlockSpec(memory_space=pl.ANY)] + [vmem] * 6,
        out_specs=(vmem,) * 5,
        scratch_shapes=[
            V((2, depth, width), bf16),
            V((n_dp, BLOCK, depth), bf16),
            V((count, depth), bf16),
            V((chunks, 2 * rank, cw), bf16),
            V((chunks, 2 * rank, cw), bf16),
            V((chunks, 2, cw), f32),
            V((chunks, 2, cw), f32),
            V((2, 2, half, rank), bf16),
            V((2, 2, half, rank), bf16),
            V((2, 2, half, rank), bf16),
            V((chunks, 2, half, cw), bf16),
            V((chunks, 2, half, cw), bf16),
            V((chunks, 2, half, cw), bf16),
            V((chunks, 2, half, cw), bf16),
            V((chunks, 2, half, cw), bf16),
            V((chunks, 2, cw), f32),
            V((chunks, 2, cw), f32),
            V((2, count + 2 * rank, cw), bf16),
            V((count, depth), f32),
            V((2, rank, depth), f32),
            V((2, count, rank), f32),
            V((2, rank, rank), f32),
            V((n_dp, BLOCK, depth), bf16),
            V((n_dp, BLOCK, depth), bf16),
            V((share, depth), f32),
            V((n_dp, share, depth), f32),
            dma((chunks, 2)),
            dma((n_dp,)), dma((n_dp,)),
            dma((messages,)), dma((messages,)),
            dma((n_dp,)), dma((n_dp,)),
            dma((n_dp,)), dma((n_dp,)),
        ],
        compiler_params=pltpu.CompilerParams(
            collective_id=0, has_side_effects=True, vmem_limit_bytes=64_000_000
        ),
        name="dora_pair",
    )(padded, frozen_weight, adapter_down, adapter_up, magnitude, hidden_gradient, gather_map, scatter_map)
    return hidden, tgrad, agrad.reshape(2, rank, depth), ugrad, mgrad


def per_device(n_dp, n_mp, *arrays):
    tokens, frozen_weight, _, adapter_up, _, hidden_gradient = arrays
    t, depth = tokens.shape
    rank, width = adapter_up.shape[1:]
    fits = (
        n_mp == 2
        and depth % TILE == 0
        and width % (CHUNKS * TILE) == 0
        and (2 * rank) % n_dp == 0
        and t + 2 * rank // n_dp <= BLOCK
        and hidden_gradient.shape[0] % 16 == 0
        and 2 * frozen_weight.size <= 24 * 2**20
    )
    if fits:
        return fused_on_device(n_dp, CHUNKS, *arrays)
    return on_device(*arrays)


CHUNKS = 3


def solution(mesh):
    in_specs = (
        P("dp", "mp"),
        P(None, "mp", "dp"),
        P(None, None, "mp"),
        P(None, None, "dp"),
        P(None, "dp"),
        P("mp", "dp"),
    )
    out_specs = (
        P("mp", "dp"),
        P("dp", "mp"),
        P(None, None, "mp"),
        P(None, None, "dp"),
        P(None, "dp"),
    )
    return jax.shard_map(
        functools.partial(per_device, mesh.shape["dp"], mesh.shape["mp"]), mesh=mesh, in_specs=in_specs, out_specs=out_specs, check_vma=False
    )
```

```python
import functools

import jax
import jax.numpy as jnp
import numpy as np
from jax import lax
from jax.experimental import pallas as pl
from jax.experimental.pallas import tpu as pltpu
from jax.sharding import PartitionSpec as P

LOWRANK_SCALE = 2.0
EPSILON = 1e-06
MATMUL_ACCURACY = lax.Precision.HIGHEST


def gelu_pair(source):
    cubic_term = source + 0.044715 * source * source * source
    tangent = jnp.tanh(0.7978845608028654 * cubic_term)
    result = 0.5 * source * (1.0 + tangent)
    derivative = 0.5 * (1.0 + tangent) + 0.5 * source * (
        1.0 - tangent * tangent
    ) * 0.7978845608028654 * (1.0 + 0.134145 * source * source)
    return (result, derivative)


def on_device(tokens, frozen_weight, adapter_down, adapter_up, magnitude, hidden_gradient):
    every_row = lax.all_gather(tokens, "dp", axis=0, tiled=True)
    down_broad = adapter_down.astype(jnp.float32)
    up_broad = adapter_up.astype(jnp.float32)
    base_square = jnp.sum(jnp.square(frozen_weight.astype(jnp.float32)), axis=1)
    cross_base = jnp.einsum(
        "krd,kdf->krf", adapter_down, frozen_weight, preferred_element_type=jnp.float32
    )
    gram_part = jnp.einsum(
        "krd,ksd->krs", adapter_down, adapter_down, preferred_element_type=jnp.float32
    )
    square_base, cross_total, gram_sum = (
        lax.psum(base_square.astype(jnp.bfloat16), "mp").astype(jnp.float32),
        lax.psum(cross_base.astype(jnp.bfloat16), "mp").astype(jnp.float32),
        lax.psum(gram_part.astype(jnp.bfloat16), "mp").astype(jnp.float32),
    )
    gram_up = jnp.einsum("krs,ksf->krf", gram_sum, up_broad, precision=MATMUL_ACCURACY)
    mixed_sum = cross_total + LOWRANK_SCALE * gram_up
    square_sum = (
        square_base
        + 2.0 * LOWRANK_SCALE * jnp.sum(up_broad * cross_total, axis=1)
        + LOWRANK_SCALE * LOWRANK_SCALE * jnp.sum(up_broad * gram_up, axis=1)
    )
    base_part = jnp.einsum(
        "td,kdf->ktf", every_row, frozen_weight, preferred_element_type=jnp.float32
    )
    lowrank_piece = jnp.einsum(
        "su,vgu->vsg", every_row, adapter_down, preferred_element_type=jnp.float32
    )
    col_norm = jnp.sqrt(square_sum + EPSILON)
    col_ratio = magnitude / col_norm
    share_rows = every_row.shape[0] // lax.axis_size("mp")
    base_sum, low_sum = (
        lax.psum(base_part.astype(jnp.bfloat16), "mp").astype(jnp.float32),
        lax.psum(lowrank_piece.astype(jnp.bfloat16), "mp").astype(jnp.float32),
    )
    cot_rows = lax.all_gather(hidden_gradient, "mp", axis=0, tiled=True)
    token_lowrank = low_sum.astype(jnp.bfloat16)
    unscaled_output = base_sum + LOWRANK_SCALE * jnp.einsum(
        "hls,hse->hle", token_lowrank, adapter_up, preferred_element_type=jnp.float32
    )
    gate_proj = unscaled_output[0] * col_ratio[0]
    up_proj = unscaled_output[1] * col_ratio[1]
    activated, derivative = gelu_pair(gate_proj)
    hidden_rows = (activated * up_proj).astype(jnp.bfloat16)
    cotangent = cot_rows.astype(jnp.float32)
    grad_out = jnp.stack([cotangent * up_proj * derivative, cotangent * activated])
    moment_part = jnp.sum(grad_out * unscaled_output, axis=1)
    prescale_gradient = (grad_out * col_ratio[:, None, :]).astype(jnp.bfloat16)
    lowrank_gradient_piece = jnp.einsum(
        "hmu,hmq->huq", token_lowrank, prescale_gradient, preferred_element_type=jnp.float32
    )
    hidden = lax.dynamic_slice_in_dim(hidden_rows, lax.axis_index("mp") * share_rows, share_rows, 0)
    magnitude_gradient = moment_part / col_norm
    frozen_term = -magnitude * moment_part / (col_norm * col_norm * col_norm)
    adapter_up_gradient = LOWRANK_SCALE * (
        lowrank_gradient_piece + mixed_sum * frozen_term[:, None, :]
    )
    lowrank_gradient = jnp.einsum(
        "pge,pbe->pgb", prescale_gradient, adapter_up, preferred_element_type=jnp.float32
    ).astype(jnp.bfloat16)
    weighted_adapter_up = up_broad * frozen_term[:, None, :]
    broadcast_value = jnp.einsum(
        "krf,kdf->krd",
        weighted_adapter_up,
        frozen_weight.astype(jnp.float32),
        precision=MATMUL_ACCURACY,
    )
    inner_gram = jnp.einsum(
        "krf,ksf->krs", weighted_adapter_up, up_broad, precision=MATMUL_ACCURACY
    )
    broadcast_value = broadcast_value + LOWRANK_SCALE * jnp.einsum(
        "krs,ksd->krd", inner_gram, down_broad, precision=MATMUL_ACCURACY
    )
    down_piece = LOWRANK_SCALE * (
        jnp.einsum("ijp,jv->ipv", lowrank_gradient, every_row, preferred_element_type=jnp.float32)
        + broadcast_value
    )
    adapter_down_gradient = lax.psum(down_piece, "dp")
    main_term = jnp.einsum(
        "ktf,kdf->td", prescale_gradient, frozen_weight, preferred_element_type=jnp.float32
    )
    token_gradient = lax.psum_scatter(
        main_term
        + LOWRANK_SCALE
        * jnp.einsum(
            "ijf,ifh->jh", lowrank_gradient, adapter_down, preferred_element_type=jnp.float32
        ),
        "dp",
        scatter_dimension=0,
        tiled=True,
    )
    return (hidden, token_gradient, adapter_down_gradient, adapter_up_gradient, magnitude_gradient)


MESH = pl.DeviceIdType.MESH
TILE = 256
LANES = 128
BLOCK = 16


def mm(left, right, precision=None):
    return lax.dot_general(
        left, right, (((1,), (0,)), ((), ())), precision=precision, preferred_element_type=jnp.float32
    )


def nt(left, right):
    return lax.dot_general(left, right, (((1,), (1,)), ((), ())), preferred_element_type=jnp.float32)


def fused_kernel(
    n_dp, chunks,
    tok, w, ad, up, mag, cot, gather_map, scatter_map,
    hid, tgrad, agrad, ugrad, mgrad,
    wv, sent, tokpad, toks, mx_s, mx_r, sq_s, sq_r, tl_s, tl_r, tl_sum,
    base_s, base_o, base_r, gp, gr, mo, mr, lhs, tacc, aacc, glow, igram,
    blk, prb, own, rsb, asum, agb,
    wsem, pr_ss, pr_rs, ag_ss, ag_rs, y_ss, y_rs, rs_ss, rs_rs, ah_ss, ah_rs,
):
    f32, bf16 = jnp.float32, jnp.bfloat16
    me = lax.axis_index("dp")
    mate = 1 - lax.axis_index("mp")
    depth, width = w.shape[1], w.shape[2]
    rank = ad.shape[1]
    half = cot.shape[0]
    cw = width // chunks
    t = tgrad.shape[0]
    share = asum.shape[0]
    side = lax.axis_index("mp")

    loads = {}
    for c in range(chunks):
        for k in range(2):
            cut = pl.ds(c * cw, cw)
            copy = pltpu.make_async_copy(w.at[k, :, cut], wv.at[k, :, cut], wsem.at[c, k])
            copy.start()
            loads[c, k] = copy

    sent[...] = jnp.concatenate([tok[...], jnp.zeros((BLOCK - t, depth), bf16)], axis=0)

    barrier = pltpu.get_barrier_semaphore()
    for i in range(1, n_dp):
        pl.semaphore_signal(barrier, inc=1, device_id={"dp": lax.rem(me + i, n_dp)}, device_id_type=MESH)
    pl.semaphore_signal(barrier, inc=1, device_id={"mp": mate}, device_id_type=MESH)
    pl.semaphore_wait(barrier, n_dp)

    chips = n_dp // 2
    chip, core = me // 2, lax.rem(me, 2)
    partner = 2 * chip + 1 - core

    def to_dp(source, target, ss, rs, i, peer):
        copy = pltpu.make_async_remote_copy(
            src_ref=source, dst_ref=target, send_sem=ss.at[i], recv_sem=rs.at[i],
            device_id={"dp": peer}, device_id_type=MESH,
        )
        copy.start()
        return copy

    def gather_start(source, target, ss, rs):
        copies = [to_dp(source, target.at[me], ss, rs, 0, partner)]
        for i in range(1, chips):
            peer = lax.rem(me + 2 * i, n_dp)
            copies.append(to_dp(source, target.at[me], ss, rs, i, peer))
        target[me] = source[...]
        return copies

    def gather_finish(copies, target, ss, rs):
        relays = []
        for i in range(1, chips):
            copies[i].wait()
            came = lax.rem(me + n_dp - 2 * i, n_dp)
            relays.append(to_dp(target.at[came], target.at[came], ss, rs, chips + i, partner))
        copies[0].wait()
        for copy in relays:
            copy.wait()

    used = []

    def to_mate(source, target):
        i = len(used)
        copy = pltpu.make_async_remote_copy(
            src_ref=source, dst_ref=target, send_sem=y_ss.at[i], recv_sem=y_rs.at[i],
            device_id={"mp": mate}, device_id_type=MESH,
        )
        used.append(copy)
        copy.start()
        return copy

    gathers = gather_start(sent, tokpad, ag_ss, ag_rs)

    stats = []
    for c in range(chunks):
        for k in range(2):
            loads[c, k].wait()
            cols = pl.ds(c * cw, cw)

            def stat_step(r, carry):
                cross, square = carry
                at = pl.ds(pl.multiple_of(r * TILE, TILE), TILE)
                piece = wv[k, at, cols]
                wide = piece.astype(f32)
                cross = cross + mm(ad[k, :, at], piece)
                square = square + jnp.sum((wide * wide).reshape(TILE // 8, 8, cw), axis=0)
                return cross, square

            cross, square = lax.fori_loop(
                0, depth // TILE, stat_step, (jnp.zeros((rank, cw), f32), jnp.zeros((8, cw), f32))
            )
            gram = nt(ad[k], ad[k])
            up32 = up[k, :, cols].astype(f32)
            gram_up = mm(gram, up32, MATMUL_ACCURACY)
            total = (
                jnp.sum(square, axis=0, keepdims=True)
                + 2.0 * LOWRANK_SCALE * jnp.sum(up32 * cross, axis=0, keepdims=True)
                + LOWRANK_SCALE * LOWRANK_SCALE * jnp.sum(up32 * gram_up, axis=0, keepdims=True)
            )
            mx_s[c, k * rank : (k + 1) * rank, :] = (cross + LOWRANK_SCALE * gram_up).astype(bf16)
            sq_s[c, k : k + 1, :] = total
        stats.append((to_mate(mx_s.at[c], mx_r.at[c]), to_mate(sq_s.at[c], sq_r.at[c])))

    gather_finish(gathers, tokpad, ag_ss, ag_rs)

    def gather_step(r, carry):
        at = pl.ds(pl.multiple_of(r * TILE, TILE), TILE)
        piece = tokpad[:, :, at].reshape(n_dp * BLOCK, TILE)
        toks[:, at] = mm(gather_map[side], piece).astype(bf16)
        return carry

    lax.fori_loop(0, depth // TILE, gather_step, 0)

    for k in range(2):
        low = nt(toks[...], ad[k]).astype(bf16)
        tl_s[0, k] = low[:half]
        tl_s[1, k] = low[half:]
    low_copy = to_mate(tl_s, tl_r)

    base_copies = []
    for c in range(chunks):

        def base_step(j, carry):
            at = pl.ds(pl.multiple_of(j * TILE, TILE), TILE)
            for k in range(2):
                piece = wv[k, :, pl.ds(pl.multiple_of(c * cw + j * TILE, TILE), TILE)]
                part = mm(toks[...], piece).astype(bf16)
                base_s[c, k, :, at] = part[:half]
                base_o[c, k, :, at] = part[half:]
            return carry

        lax.fori_loop(0, cw // TILE, base_step, 0)
        base_copies.append(to_mate(base_s.at[c], base_r.at[c]))

    low_copy.wait()
    for k in range(2):
        tl_sum[0, k] = (tl_s[0, k].astype(f32) + tl_r[1, k].astype(f32)).astype(bf16)
        tl_sum[1, k] = (tl_s[1, k].astype(f32) + tl_r[0, k].astype(f32)).astype(bf16)

    grads = []
    for c in range(chunks):
        for copy in stats[c]:
            copy.wait()
        base_copies[c].wait()

        def point_step(j, carry):
            at = pl.ds(pl.multiple_of(j * LANES, LANES), LANES)
            wide_at = pl.ds(pl.multiple_of(c * cw + j * LANES, LANES), LANES)
            pres, ratios = [], []
            for k in range(2):
                norm = jnp.sqrt(sq_s[c, k : k + 1, at] + sq_r[c, k : k + 1, at] + EPSILON)
                ratios.append(mag[k : k + 1, wide_at] / norm)
                base = base_o[c, k, :, at].astype(f32) + base_r[c, k, :, at].astype(f32)
                pres.append(base + LOWRANK_SCALE * mm(tl_sum[1, k], up[k, :, wide_at]))
            gate, upper = pres[0] * ratios[0], pres[1] * ratios[1]
            activated, derivative = gelu_pair(gate)
            hid[:, wide_at] = (activated * upper).astype(bf16)
            cotangent = cot[:, wide_at].astype(f32)
            outs = (cotangent * upper * derivative, cotangent * activated)
            for k in range(2):
                mo[c, k : k + 1, at] = jnp.sum(outs[k] * pres[k], axis=0, keepdims=True)
                gp[c, k, :, at] = (outs[k] * ratios[k]).astype(bf16)
            return carry

        lax.fori_loop(0, cw // LANES, point_step, 0)
        grads.append((to_mate(gp.at[c], gr.at[c]), to_mate(mo.at[c], mr.at[c])))

    for c in range(chunks):
        for copy in grads[c]:
            copy.wait()
        cols = pl.ds(c * cw, cw)
        for k in range(2):
            moment = mo[c, k : k + 1, :] + mr[c, k : k + 1, :]
            norm = jnp.sqrt(sq_s[c, k : k + 1, :] + sq_r[c, k : k + 1, :] + EPSILON)
            mgrad[k : k + 1, cols] = moment / norm
            frozen_term = -mag[k : k + 1, cols] * moment / (norm * norm * norm)
            part = pl.ds(k * rank, rank)
            mixed = mx_s[c, part, :].astype(f32) + mx_r[c, part, :].astype(f32)
            up16 = up[k, :, cols]
            weighted = up16.astype(f32) * frozen_term
            high = weighted.astype(bf16)
            low = (weighted - high.astype(f32)).astype(bf16)
            theirs, mine = gr[c, k], gp[c, k]
            piece = mm(tl_sum[0, k].astype(f32).T.astype(bf16), theirs) + mm(
                tl_sum[1, k].astype(f32).T.astype(bf16), mine
            )
            ugrad[k, :, cols] = LOWRANK_SCALE * (piece + mixed * frozen_term)
            lhs[k, 0:half, :] = theirs
            lhs[k, half : 2 * half, :] = mine
            lhs[k, 2 * half : 2 * half + rank, :] = high
            lhs[k, 2 * half + rank : 2 * half + 2 * rank, :] = low
            small = nt(lhs[k], up16)
            gl, ig = small[: 2 * half], small[2 * half : 2 * half + rank] + small[2 * half + rank :]
            if c == 0:
                glow[k] = gl
                igram[k] = ig
            else:
                glow[k] += gl
                igram[k] += ig

        def grad_step(r, carry):
            at = pl.ds(pl.multiple_of(r * TILE, TILE), TILE)
            outs = [nt(lhs[k], wv[k, at, cols]) for k in range(2)]
            main = outs[0][: 2 * half] + outs[1][: 2 * half]
            if c == 0:
                tacc[:, at] = main
            else:
                tacc[:, at] += main
            for k in range(2):
                spread = outs[k][2 * half : 2 * half + rank] + outs[k][2 * half + rank :]
                if c == 0:
                    aacc[k, :, at] = spread
                else:
                    aacc[k, :, at] += spread
            return carry

        lax.fori_loop(0, depth // TILE, grad_step, 0)

    def final_step(r, carry):
        at = pl.ds(pl.multiple_of(r * TILE, TILE), TILE)
        main = tacc[:, at]
        parts = []
        for k in range(2):
            low = glow[k].astype(bf16)
            adt = ad[k, :, at]
            main = main + LOWRANK_SCALE * mm(low, adt)
            spread = aacc[k, :, at] + LOWRANK_SCALE * mm(igram[k], adt.astype(f32), MATMUL_ACCURACY)
            parts.append(LOWRANK_SCALE * (mm(glow[k].T.astype(bf16), toks[:, at]) + spread))
        whole = jnp.concatenate([main] + parts, axis=0).astype(bf16)
        packed = mm(scatter_map[side], whole).astype(bf16)
        blk[:, :, at] = packed.reshape(n_dp, BLOCK, TILE)
        return carry

    tiles = depth // TILE // CUTS
    pairs = []
    for q in range(CUTS):
        lax.fori_loop(q * tiles, (q + 1) * tiles, final_step, 0)
        cut = pl.ds(q * tiles * TILE, tiles * TILE)
        pairs.append(to_dp(blk.at[pl.ds((1 - core) * chips, chips), :, cut], prb.at[:, :, cut], pr_ss, pr_rs, q, partner))

    scatters = []
    for q in range(CUTS):
        pairs[q].wait()

        def pair_step(r, carry):
            at = pl.ds(pl.multiple_of(r * TILE, TILE), TILE)
            for j in range(chips):
                total = blk[core * chips + j, :, at].astype(f32) + prb[j, :, at].astype(f32)
                own[j, :, at] = total.astype(bf16)
            return carry

        lax.fori_loop(q * tiles, (q + 1) * tiles, pair_step, 0)
        cut = pl.ds(q * tiles * TILE, tiles * TILE)
        sends = []
        for i in range(1, chips):
            there = lax.rem(chip + i, chips)
            sends.append(
                to_dp(own.at[there, :, cut], rsb.at[i, :, cut], rs_ss, rs_rs, q * chips + i, 2 * there + core)
            )
        scatters.append(sends)

    for q in range(CUTS):
        for copy in scatters[q]:
            copy.wait()

        def sum_step(r, carry):
            at = pl.ds(pl.multiple_of(r * TILE, TILE), TILE)
            total = own[chip, :, at].astype(f32)
            for i in range(1, chips):
                total = total + rsb[i, :, at].astype(f32)
            tgrad[:, at] = total[:t]
            asum[:, at] = total[t : t + share].astype(bf16)
            return carry

        lax.fori_loop(q * tiles, (q + 1) * tiles, sum_step, 0)

    spreads = gather_start(asum, agb, ah_ss, ah_rs)
    gather_finish(spreads, agb, ah_ss, ah_rs)
    for b in range(n_dp):
        k, row = (b * share) // rank, (b * share) % rank
        agrad[k, row : row + share, :] = agb[b].astype(f32)


def copy_kernel(*refs):
    for source, target in zip(refs[:5], refs[5:]):
        target[...] = source[...]


def fused_on_device(n_dp, chunks, tokens, frozen_weight, adapter_down, adapter_up, magnitude, hidden_gradient):
    f32, bf16 = jnp.float32, jnp.bfloat16
    t, depth = tokens.shape
    rank, width = adapter_up.shape[1:]
    half = hidden_gradient.shape[0]
    count = n_dp * t
    share = 2 * rank // n_dp
    cw = width // chunks
    slots = np.arange(n_dp * BLOCK)
    by_core = lambda block: (block % 2) * (n_dp // 2) + block // 2
    spots = np.arange(2 * rank)
    spots = by_core(spots // share) * BLOCK + t + spots % share
    gathers, scatters = [], []
    for side in range(2):
        order = (np.arange(count) + (1 - side) * half) % count
        places = (order // t) * BLOCK + order % t
        homes = by_core(order // t) * BLOCK + order % t
        gathers.append(places[:, None] == slots[None, :])
        scatters.append(slots[:, None] == np.concatenate([homes, spots])[None, :])
    gather_map = jnp.asarray(np.stack(gathers), bf16)
    scatter_map = jnp.asarray(np.stack(scatters), bf16)
    vmem = pl.BlockSpec(memory_space=pltpu.VMEM)
    dma = pltpu.SemaphoreType.DMA
    V = pltpu.VMEM
    messages = 5 * chunks + 1 + chunks
    shapes = (
        jax.ShapeDtypeStruct((half, width), bf16),
        jax.ShapeDtypeStruct((t, depth), f32),
        jax.ShapeDtypeStruct((2, rank, depth), f32),
        jax.ShapeDtypeStruct((2, rank, width), f32),
        jax.ShapeDtypeStruct((2, width), f32),
    )
    outs = pl.pallas_call(
        functools.partial(fused_kernel, n_dp, chunks),
        out_shape=shapes,
        in_specs=[vmem, pl.BlockSpec(memory_space=pl.ANY)] + [vmem] * 6,
        out_specs=(vmem,) * 5,
        scratch_shapes=[
            V((2, depth, width), bf16),
            V((BLOCK, depth), bf16),
            V((n_dp, BLOCK, depth), bf16),
            V((count, depth), bf16),
            V((chunks, 2 * rank, cw), bf16),
            V((chunks, 2 * rank, cw), bf16),
            V((chunks, 2, cw), f32),
            V((chunks, 2, cw), f32),
            V((2, 2, half, rank), bf16),
            V((2, 2, half, rank), bf16),
            V((2, 2, half, rank), bf16),
            V((chunks, 2, half, cw), bf16),
            V((chunks, 2, half, cw), bf16),
            V((chunks, 2, half, cw), bf16),
            V((chunks, 2, half, cw), bf16),
            V((chunks, 2, half, cw), bf16),
            V((chunks, 2, cw), f32),
            V((chunks, 2, cw), f32),
            V((2, count + 2 * rank, cw), bf16),
            V((count, depth), f32),
            V((2, rank, depth), f32),
            V((2, count, rank), f32),
            V((2, rank, rank), f32),
            V((n_dp, BLOCK, depth), bf16),
            V((n_dp // 2, BLOCK, depth), bf16),
            V((n_dp // 2, BLOCK, depth), bf16),
            V((n_dp // 2, BLOCK, depth), bf16),
            V((share, depth), bf16),
            V((n_dp, share, depth), bf16),
            dma((chunks, 2)),
            dma((CUTS,)), dma((CUTS,)),
            dma((n_dp,)), dma((n_dp,)),
            dma((messages,)), dma((messages,)),
            dma((CUTS * n_dp // 2,)), dma((CUTS * n_dp // 2,)),
            dma((n_dp,)), dma((n_dp,)),
        ],
        compiler_params=pltpu.CompilerParams(
            collective_id=0, has_side_effects=True, vmem_limit_bytes=64_000_000
        ),
        name="dora_pair",
    )(tokens, frozen_weight, adapter_down, adapter_up, magnitude, hidden_gradient, gather_map, scatter_map)
    return pl.pallas_call(
        copy_kernel, out_shape=shapes, in_specs=[vmem] * 5, out_specs=(vmem,) * 5, name="hand_over"
    )(*outs)


def per_device(n_dp, n_mp, *arrays):
    tokens, frozen_weight, _, adapter_up, _, hidden_gradient = arrays
    t, depth = tokens.shape
    rank, width = adapter_up.shape[1:]
    fits = (
        n_mp == 2
        and n_dp % 2 == 0
        and depth % (CUTS * TILE) == 0
        and width % (CHUNKS * TILE) == 0
        and (2 * rank) % n_dp == 0
        and rank % (2 * rank // n_dp) == 0
        and t + 2 * rank // n_dp <= BLOCK
        and hidden_gradient.shape[0] % 16 == 0
        and 2 * frozen_weight.size <= 24 * 2**20
    )
    if fits:
        return fused_on_device(n_dp, CHUNKS, *arrays)
    return on_device(*arrays)


CHUNKS = 3
CUTS = 3


def solution(mesh):
    in_specs = (
        P("dp", "mp"),
        P(None, "mp", "dp"),
        P(None, None, "mp"),
        P(None, None, "dp"),
        P(None, "dp"),
        P("mp", "dp"),
    )
    out_specs = (
        P("mp", "dp"),
        P("dp", "mp"),
        P(None, None, "mp"),
        P(None, None, "dp"),
        P(None, "dp"),
    )
    return jax.shard_map(
        functools.partial(per_device, mesh.shape["dp"], mesh.shape["mp"]), mesh=mesh, in_specs=in_specs, out_specs=out_specs, check_vma=False
    )
```
